32 devices in a mesh: doc: 2 (over x), seq: 16 (over z, y, core).
Axes of the slice: x: 2, y: 2, z: 4, core: 2. Of those that a mesh axis runs over, the one named last changes fastest.
Arguments:
- queries: bfloat16 [4096, 1792], P(('doc', 'seq')), parts along dimension 0, may hold values from -5 to 5
- keys: bfloat16 [4096, 256], P(('doc', 'seq')), parts along dimension 0, may hold values from -5 to 5
- values: bfloat16 [4096, 256], P(('doc', 'seq')), parts along dimension 0, may hold values from -6 to 6
- doc_length: int32 [2], P('doc'), parts along dimension 0, may hold values from 1024 to 2048
- sink_pos: int32 [8], P('doc'), parts along dimension 0, may hold values from 0 to 127, as said below
Outputs:
- attended: bfloat16 [4096, 1792], P(('doc', 'seq')), parts along dimension 0
- row_lse: float32 [14, 4096], P(None, ('doc', 'seq')), parts along dimension 1
- sink_mass: float32 [14, 4096], P(None, ('doc', 'seq')), parts along dimension 1
- head_lse: float32 [28], P('doc'), parts along dimension 0
- head_sink: float32 [28], P('doc'), parts along dimension 0
The draws below stay inside these ranges and needn't reach their ends.
There are 2 independent parts, one for each index of `doc`. The reference program is written for one: setup_inputs(seed, part) draws one part's arguments, and reference() takes and returns one part's arrays. A program takes and returns all parts, laid end to end along the dimension named above; each array names one. Nothing has to cross between parts.
Inputs may be any that keep to these rules, and one draw needn't show every extreme that they name: `sink_pos`: 4 distinct positions within the document's first 128 tokens; positions 0 and 127 are always among them. Positions from doc_length up to 2048 are padding.
All inputs are finite; a program needn't handle non-finite values.
Results may differ from the reference program's by a relative error of at most 0.009.
Values may be sent and summed in bfloat16 or wider, within the bound.
A program may use at most 64 MiB of HBM per device.

```python
import jax
import jax.numpy as jnp
from jax import lax

QUERY_HEADS = 14
KEY_VALUE_HEADS = 2
HEAD_DIMENSION = 128
NSINK = 4
S_DEV = 128
PADDED_LENGTH = 2048


def draw_queries(key, part):
    query_group_width = QUERY_HEADS // KEY_VALUE_HEADS
    unsharded_result = jnp.clip(jax.random.normal(jax.random.fold_in(key, 11), (PADDED_LENGTH, KEY_VALUE_HEADS, query_group_width, HEAD_DIMENSION), jnp.float32), -5.0, 5.0)
    return unsharded_result.reshape(PADDED_LENGTH, QUERY_HEADS * HEAD_DIMENSION).astype(jnp.bfloat16)


def draw_keys(key, part):
    unsharded_result = jnp.clip(jax.random.normal(jax.random.fold_in(key, 13), (PADDED_LENGTH, KEY_VALUE_HEADS, HEAD_DIMENSION), jnp.float32), -5.0, 5.0)
    return unsharded_result.reshape(PADDED_LENGTH, KEY_VALUE_HEADS * HEAD_DIMENSION).astype(jnp.bfloat16)


def draw_sink_pos(key, part):
    order = jax.random.permutation(jax.random.fold_in(key, 17), S_DEV - 2)
    middle = order[:NSINK - 2].astype(jnp.int32) + 1
    first = jnp.zeros((1,), jnp.int32)
    last = jnp.full((1,), S_DEV - 1, jnp.int32)
    return jnp.concatenate([first, middle, last]).astype(jnp.int32)


def level_of(key, extent, split, low, top_value):
    loudness, own = 1.0, jax.random.fold_in(key, 6)
    for dim, shards_of in split:
        draws = jnp.exp(jax.random.uniform(jax.random.fold_in(own, dim), (shards_of,), jnp.float32, low / len(split), top_value / len(split)))
        loudness = loudness * jnp.repeat(draws, extent[dim] // shards_of).reshape([-1 if axis == dim else 1 for axis in range(len(extent))])
    return loudness


def scatter_about(rng, extent, deviation, most, pieces=(), kind=jnp.bfloat16):
    drawn = jax.random.normal(rng, extent, jnp.float32) * deviation
    if len(pieces) > 0:
        drawn = level_of(rng, extent, pieces, -0.22, 0.18) * drawn
    return jnp.clip(drawn, min=-most, max=most).astype(kind)


def setup_inputs(seed: int = 0, part: int = 0) -> dict:
    splits = jax.random.split(jax.random.key(seed), 6)
    own_keys = jax.random.split(jax.random.fold_in(splits[5], part), 6)
    return {
        "queries": draw_queries(jax.random.fold_in(jax.random.fold_in(splits[5], part), 71), part),
        "keys": draw_keys(jax.random.fold_in(jax.random.fold_in(splits[5], part), 71), part),
        "values": scatter_about(own_keys[2], (PADDED_LENGTH, KEY_VALUE_HEADS * HEAD_DIMENSION), 1.0, 6.0, ((0, 16),)),
        "doc_length": jax.random.randint(own_keys[3], (1,), PADDED_LENGTH // 2, PADDED_LENGTH + 1).astype(jnp.int32),
        "sink_pos": draw_sink_pos(jax.random.fold_in(jax.random.fold_in(splits[5], part), 71), part),
    }


def reference(queries, keys, values, doc_length, sink_pos):
    query_group_width = QUERY_HEADS // KEY_VALUE_HEADS
    length = doc_length[0]
    key_float = keys.reshape(PADDED_LENGTH, KEY_VALUE_HEADS, HEAD_DIMENSION).astype(jnp.float32)
    value_float = values.reshape(PADDED_LENGTH, KEY_VALUE_HEADS, HEAD_DIMENSION).astype(jnp.float32)
    key_pos = jnp.arange(PADDED_LENGTH, dtype=jnp.int32)
    is_sink = jnp.any(key_pos[:, None] == sink_pos[None, :], axis=1)
    rows_per_block = min(512, PADDED_LENGTH)
    block_count = PADDED_LENGTH // rows_per_block
    score_scale = HEAD_DIMENSION ** -0.5

    def one_block(block_index):
        first = (block_index * rows_per_block).astype(jnp.int32)
        query_float = lax.dynamic_slice_in_dim(queries, first, rows_per_block, 0)
        query_float = query_float.reshape(rows_per_block, KEY_VALUE_HEADS, query_group_width, HEAD_DIMENSION).astype(jnp.float32)
        scores = jnp.einsum("sgcd,pgd->gcsp", query_float, key_float, precision=lax.Precision.HIGHEST) * score_scale
        query_pos = first + jnp.arange(rows_per_block, dtype=jnp.int32)
        allowed = (key_pos[None, :] <= query_pos[:, None]) & (key_pos[None, :] < length)
        masked = jnp.where(allowed, scores, -jnp.inf)
        peak = jnp.max(masked, axis=-1, keepdims=True)
        row_lse = peak[..., 0] + jnp.log(jnp.sum(jnp.exp(masked - peak), axis=-1))
        probs = jnp.exp(masked - row_lse[..., None])
        sink_mass = jnp.sum(jnp.where(is_sink, probs, 0.0), axis=-1)
        rounded = lax.optimization_barrier(probs.astype(jnp.bfloat16)).astype(jnp.float32)
        attended = jnp.einsum("gcsp,pgd->sgcd", rounded, value_float, precision=lax.Precision.HIGHEST)
        attended = attended.reshape(rows_per_block, QUERY_HEADS * HEAD_DIMENSION)
        live_rows = query_pos < length
        attended = jnp.where(live_rows[:, None], attended, 0.0).astype(jnp.bfloat16)
        row_lse = jnp.where(live_rows[None, :], row_lse.reshape(QUERY_HEADS, rows_per_block), 0.0)
        sink_mass = jnp.where(live_rows[None, :], sink_mass.reshape(QUERY_HEADS, rows_per_block), 0.0)
        return attended, row_lse, sink_mass

    attended, row_lse, sink_mass = lax.map(one_block, jnp.arange(block_count, dtype=jnp.int32))
    attended = attended.reshape(PADDED_LENGTH, QUERY_HEADS * HEAD_DIMENSION)
    row_lse = row_lse.transpose(1, 0, 2).reshape(QUERY_HEADS, PADDED_LENGTH)
    sink_mass = sink_mass.transpose(1, 0, 2).reshape(QUERY_HEADS, PADDED_LENGTH)
    doc_count = length.astype(jnp.float32)
    head_lse = jnp.sum(row_lse, axis=1) / doc_count
    head_sink = jnp.sum(sink_mass, axis=1) / doc_count
    return (attended, row_lse, sink_mass, head_lse, head_sink)
```

```python
import functools
import math

import jax
import jax.numpy as jnp
from jax import lax
from jax.experimental import pallas as pl
from jax.experimental.pallas import tpu as pltpu
from jax.sharding import PartitionSpec as P

HEAD_DIMENSION = 128
PLANE = 4
EXTRA = 16
MESH = pl.DeviceIdType.MESH
NEG = -1e30


def kernel(
    n, rows, heads, groups,
    len_ref, sink_ref, q_hbm, k_ref, v_ref,
    out_hbm, rl_ref, sm_ref, hd_ref,
    qb, kb, vb, vt, acc, mref, ob, stat_x, stat_tx, stat_rx,
    qsem, osem, ssem, rsem, tsem, usem,
):
    hd = HEAD_DIMENSION
    planes = n // PLANE
    span = PLANE * rows
    width = heads // groups
    me = lax.axis_index("seq")
    z = me // PLANE
    y = (me // 2) % 2
    c = me % 2
    scale = (hd ** -0.5) * math.log2(math.e)

    def block_id(p, yy, cc):
        return p * PLANE + yy * 2 + cc

    def block(ref, b):
        return ref.at[pl.ds(pl.multiple_of(b * rows, rows), rows)]

    ports = ((k_ref, kb, 0), (v_ref, vb, 1))

    def move(b, dev, slot, own=False):
        return [
            pltpu.make_async_remote_copy(
                src_ref=src if own else block(buf, b),
                dst_ref=block(buf, b),
                send_sem=ssem.at[kind, slot],
                recv_sem=rsem.at[kind, b],
                device_id={"seq": dev},
                device_id_type=MESH,
            )
            for src, buf, kind in ports
        ]

    def arrive(b, dev):
        return move(b, dev, 0)

    def slot_z(p):
        return p

    def slot_y(p):
        return planes + p

    def slot_c(p, k):
        return 2 * planes + 2 * p + k

    y_dev = block_id(z, 1 - y, c)
    c_dev = block_id(z, y, 1 - c)

    barrier = pltpu.get_barrier_semaphore()

    def greet(i, carry):
        pl.semaphore_signal(
            barrier, inc=1, device_id={"seq": (me + i) % n}, device_id_type=MESH
        )
        return carry

    lax.fori_loop(1, n, greet, 0)

    def q_copy(h):
        return pltpu.make_async_copy(
            q_hbm.at[:, pl.ds(h * hd, hd)], qb.at[pl.ds(h * rows, rows)], qsem.at[h]
        )

    for h in range(heads):
        q_copy(h).start()
    block(kb, me)[...] = k_ref[...]
    block(vb, me)[...] = v_ref[...]
    pl.semaphore_wait(barrier, n - 1)

    for copy in move(me, y_dev, slot_y(z), own=True):
        copy.start()
    for copy in move(me, c_dev, slot_c(z, 0), own=True):
        copy.start()

    def z_send(p):
        return move(me, block_id(p, y, c), slot_z(p), own=True)

    def send_up(i, carry):
        for copy in z_send(planes - 1 - i):
            copy.start()
        return carry

    lax.fori_loop(0, planes - 1 - z, send_up, 0)

    def take_z(p):
        b = block_id(p, y, c)
        for got, to_y, to_c in zip(
            arrive(b, y_dev), move(b, y_dev, slot_y(p)), move(b, c_dev, slot_c(p, 0))
        ):
            got.wait_recv()
            to_y.start()
            to_c.start()

    def take_y(p):
        b = block_id(p, 1 - y, c)
        for got, to_c in zip(arrive(b, y_dev), move(b, c_dev, slot_c(p, 1))):
            got.wait_recv()
            to_c.start()

    def take_c(p):
        for yy in (y, 1 - y):
            for got in arrive(block_id(p, yy, 1 - c), c_dev):
                got.wait_recv()

    def compute(p, g, first):
        base = pl.multiple_of(p * span, span)
        kp = kb[pl.ds(base, span), g * hd : (g + 1) * hd]
        vt[g, 0:hd, :] = vb[pl.ds(base, span), g * hd : (g + 1) * hd].T
        lane = lax.broadcasted_iota(jnp.int32, (EXTRA, span), 1) + base
        sub = lax.broadcasted_iota(jnp.int32, (EXTRA, span), 0)
        is_sink = lane == sink_ref[0]
        for i in range(1, sink_ref.shape[0]):
            is_sink = is_sink | (lane == sink_ref[i])
        marks = jnp.where(sub == 0, 1.0, jnp.where((sub == 1) & is_sink, 1.0, 0.0))
        vt[g, hd : hd + EXTRA, :] = marks.astype(jnp.bfloat16)
        vtg = vt[g]
        for h0 in range(0, width, 2):
            w = min(2, width - h0) * rows
            c0 = (g * width + h0) * rows
            cols = slice(c0, c0 + w)
            s = lax.dot_general(
                kp, qb[cols, :], (((1,), (1,)), ((), ())),
                preferred_element_type=jnp.float32,
            )
            if first:
                key_pos = base + lax.broadcasted_iota(jnp.int32, (span, w), 0)
                row = lax.broadcasted_iota(jnp.int32, (span, w), 1) % rows
                s = jnp.where(key_pos <= me * rows + row, s, NEG)
            top = jnp.max(s, axis=0, keepdims=True) * scale
            if first:
                new = top
            else:
                old = mref[:, cols]
                new = jnp.maximum(old, top)
            prob = jnp.exp2(s * scale - new).astype(jnp.bfloat16)
            part = jnp.dot(vtg, prob, preferred_element_type=jnp.float32)
            if first:
                acc[:, cols] = part
            else:
                acc[:, cols] = acc[:, cols] * jnp.exp2(old - new) + part
            mref[:, cols] = new

    take_y(z)
    for h in range(heads):
        q_copy(h).wait()
    take_c(z)

    def step(p, first):
        more = p > 0

        @pl.when(more)
        def _():
            take_z(p - 1)

        for g in range(groups):
            compute(p, g, first)
            if g == 0:
                @pl.when(more)
                def _():
                    take_y(p - 1)

        @pl.when(more)
        def _():
            take_c(p - 1)

    step(z, True)

    def body(t, carry):
        step(z - t, False)
        return carry

    lax.fori_loop(1, z + 1, body, 0)

    length = len_ref[0]
    live = (me * rows + lax.broadcasted_iota(jnp.int32, (1, rows), 1)) < length
    stat_x[...] = jnp.zeros_like(stat_x)
    for h in range(heads):
        cols = slice(h * rows, (h + 1) * rows)
        total = acc[hd : hd + 1, cols]
        lse = (mref[:, cols] + jnp.log2(total)) * math.log(2.0)
        lse = jnp.where(live, lse, 0.0)
        mass = jnp.where(live, acc[hd + 1 : hd + 2, cols] / total, 0.0)
        rl_ref[h : h + 1, :] = lse
        sm_ref[h : h + 1, :] = mass
        stat_x[h : h + 1, :] = lse
        stat_x[64 + h : 65 + h, :] = mass
    sums = lax.dot_general(
        jnp.ones((8, rows), jnp.float32), stat_x[...], (((1,), (1,)), ((), ())),
        precision=lax.Precision.HIGHEST, preferred_element_type=jnp.float32,
    )
    stat_tx[...] = sums[0:1]

    def stat_copy(i):
        dev = (me + i) % n
        return pltpu.make_async_remote_copy(
            src_ref=stat_tx,
            dst_ref=stat_rx.at[me],
            send_sem=tsem.at[i],
            recv_sem=usem.at[me],
            device_id={"seq": dev},
            device_id_type=MESH,
        )

    def stat_from(i):
        src = (me + i) % n
        return pltpu.make_async_remote_copy(
            src_ref=stat_tx,
            dst_ref=stat_rx.at[src],
            send_sem=tsem.at[i],
            recv_sem=usem.at[src],
            device_id={"seq": src},
            device_id_type=MESH,
        )

    def stat_start(i, carry):
        stat_copy(i).start()
        return carry

    lax.fori_loop(1, n, stat_start, 0)

    def o_copy(h):
        return pltpu.make_async_copy(
            ob.at[:, pl.ds(h * hd, hd)], out_hbm.at[:, pl.ds(h * hd, hd)], osem.at[h]
        )

    for h in range(heads):
        cols = slice(h * rows, (h + 1) * rows)
        inv = jnp.where(live, 1.0 / acc[hd : hd + 1, cols], 0.0)
        ob[:, h * hd : (h + 1) * hd] = (acc[0:hd, cols] * inv).T.astype(jnp.bfloat16)
        o_copy(h).start()

    def z_done(p, carry):
        for copy in z_send(p):
            copy.wait_send()
        return carry

    lax.fori_loop(z + 1, planes, z_done, 0)

    def yc_done(p, carry):
        for copy in move(block_id(p, y, c), y_dev, slot_y(p)):
            copy.wait_send()
        for k in range(2):
            for copy in move(block_id(p, y, c), c_dev, slot_c(p, k)):
                copy.wait_send()
        return carry

    lax.fori_loop(0, z + 1, yc_done, 0)

    def stat_wait(i, carry):
        stat_copy(i).wait_send()
        stat_from(i).wait_recv()
        return carry

    lax.fori_loop(1, n, stat_wait, 0)
    stat_rx[pl.ds(me, 1)] = stat_tx[...].reshape(1, 1, rows)
    hd_ref[...] = jnp.sum(stat_rx[...], axis=0) / length.astype(jnp.float32)
    for h in range(heads):
        o_copy(h).wait()


def body(n, queries, keys, values, doc_length, sink_pos):
    rows, qcols = queries.shape
    kcols = keys.shape[1]
    heads = qcols // HEAD_DIMENSION
    groups = kcols // HEAD_DIMENSION
    planes = n // PLANE
    f32, bf16 = jnp.float32, jnp.bfloat16
    smem = pl.BlockSpec(memory_space=pltpu.SMEM)
    vmem = pl.BlockSpec(memory_space=pltpu.VMEM)
    hbm = pl.BlockSpec(memory_space=pl.ANY)
    attended, row_lse, sink_mass, head = pl.pallas_call(
        functools.partial(kernel, n, rows, heads, groups),
        out_shape=(
            jax.ShapeDtypeStruct((rows, qcols), bf16),
            jax.ShapeDtypeStruct((heads, rows), f32),
            jax.ShapeDtypeStruct((heads, rows), f32),
            jax.ShapeDtypeStruct((1, 128), f32),
        ),
        in_specs=[smem, smem, hbm, vmem, vmem],
        out_specs=(hbm, vmem, vmem, vmem),
        scratch_shapes=[
            pltpu.VMEM((heads * rows, HEAD_DIMENSION), bf16),
            pltpu.VMEM((n * rows, kcols), bf16),
            pltpu.VMEM((n * rows, kcols), bf16),
            pltpu.VMEM((groups, HEAD_DIMENSION + EXTRA, PLANE * rows), bf16),
            pltpu.VMEM((HEAD_DIMENSION + EXTRA, heads * rows), f32),
            pltpu.VMEM((1, heads * rows), f32),
            pltpu.VMEM((rows, qcols), bf16),
            pltpu.VMEM((128, rows), f32),
            pltpu.VMEM((1, 128), f32),
            pltpu.VMEM((n, 1, 128), f32),
            pltpu.SemaphoreType.DMA((heads,)),
            pltpu.SemaphoreType.DMA((heads,)),
            pltpu.SemaphoreType.DMA((2, 4 * planes)),
            pltpu.SemaphoreType.DMA((2, n)),
            pltpu.SemaphoreType.DMA((n,)),
            pltpu.SemaphoreType.DMA((n,)),
        ],
        compiler_params=pltpu.CompilerParams(collective_id=0, has_side_effects=True),
    )(doc_length, sink_pos, queries, keys, values)
    return attended, row_lse, sink_mass, head[0, :heads], head[0, 64 : 64 + heads]


def solution(mesh):
    placed = (
        P(("doc", "seq"), None),
        P(("doc", "seq"), None),
        P(("doc", "seq"), None),
        P("doc"),
        P("doc"),
    )
    return jax.shard_map(
        functools.partial(body, mesh.shape["seq"]),
        mesh=mesh,
        in_specs=placed,
        out_specs=(
            P(("doc", "seq"), None),
            P(None, ("doc", "seq")),
            P(None, ("doc", "seq")),
            P("doc"),
            P("doc"),
        ),
        check_vma=False,
    )
```

```python
import functools
import math

import jax
import jax.numpy as jnp
from jax import lax
from jax.experimental import pallas as pl
from jax.experimental.pallas import tpu as pltpu
from jax.sharding import PartitionSpec as P

HEAD_DIMENSION = 128
PLANE = 4
EXTRA = 16
MESH = pl.DeviceIdType.MESH
NEG = -1e30


def kernel(
    n, rows, heads, groups,
    len_ref, sink_ref, q_hbm, k_ref, v_ref,
    out_ref, rl_ref, sm_ref, hd_ref,
    qb, kb, vb, vt, acc, mref, stat_x, stat_tx, stat_rx,
    qsem, ssem, rsem, tsem, usem,
):
    hd = HEAD_DIMENSION
    planes = n // PLANE
    span = PLANE * rows
    width = heads // groups
    me = lax.axis_index("seq")
    z = me // PLANE
    y = (me // 2) % 2
    c = me % 2
    scale = (hd ** -0.5) * math.log2(math.e)

    def block_id(p, yy, cc):
        return p * PLANE + yy * 2 + cc

    def block(ref, b):
        return ref.at[pl.ds(pl.multiple_of(b * rows, rows), rows)]

    ports = ((k_ref, kb, 0), (v_ref, vb, 1))

    def move(b, dev, slot, own=False):
        return [
            pltpu.make_async_remote_copy(
                src_ref=src if own else block(buf, b),
                dst_ref=block(buf, b),
                send_sem=ssem.at[kind, slot],
                recv_sem=rsem.at[kind, b],
                device_id={"seq": dev},
                device_id_type=MESH,
            )
            for src, buf, kind in ports
        ]

    def arrive(b, dev):
        return move(b, dev, 0)

    def slot_z(p):
        return p

    def slot_y(p):
        return planes + p

    def slot_c(p, k):
        return 2 * planes + 2 * p + k

    y_dev = block_id(z, 1 - y, c)
    c_dev = block_id(z, y, 1 - c)

    barrier = pltpu.get_barrier_semaphore()

    def greet(i, carry):
        pl.semaphore_signal(
            barrier, inc=1, device_id={"seq": (me + i) % n}, device_id_type=MESH
        )
        return carry

    lax.fori_loop(1, n, greet, 0)

    def q_copy(h):
        return pltpu.make_async_copy(
            q_hbm.at[:, pl.ds(h * hd, hd)], qb.at[pl.ds(h * rows, rows)], qsem.at[h]
        )

    for h in range(heads):
        q_copy(h).start()
    block(kb, me)[...] = k_ref[...]
    block(vb, me)[...] = v_ref[...]
    pl.semaphore_wait(barrier, n - 1)

    up_dev = block_id(z + 1, y, c)
    has_up = z + 1 < planes

    @pl.when(has_up)
    def _():
        for copy in move(me, up_dev, slot_z(z), own=True):
            copy.start()

    for copy in move(me, y_dev, slot_y(z), own=True):
        copy.start()
    for copy in move(me, c_dev, slot_c(z, 0), own=True):
        copy.start()

    def take_z(p):
        b = block_id(p, y, c)
        for got, to_z, to_y, to_c in zip(
            arrive(b, y_dev),
            move(b, up_dev, slot_z(p)),
            move(b, y_dev, slot_y(p)),
            move(b, c_dev, slot_c(p, 0)),
        ):
            got.wait_recv()
            pl.when(has_up)(to_z.start)
            to_y.start()
            to_c.start()

    def take_y(p):
        b = block_id(p, 1 - y, c)
        for got, to_c in zip(arrive(b, y_dev), move(b, c_dev, slot_c(p, 1))):
            got.wait_recv()
            to_c.start()

    def take_c(p):
        for yy in (y, 1 - y):
            for got in arrive(block_id(p, yy, 1 - c), c_dev):
                got.wait_recv()

    def compute(p, g, first):
        base = pl.multiple_of(p * span, span)
        kp = kb[pl.ds(base, span), g * hd : (g + 1) * hd]
        vt[g, 0:hd, :] = vb[pl.ds(base, span), g * hd : (g + 1) * hd].T
        lane = lax.broadcasted_iota(jnp.int32, (EXTRA, span), 1) + base
        sub = lax.broadcasted_iota(jnp.int32, (EXTRA, span), 0)
        is_sink = lane == sink_ref[0]
        for i in range(1, sink_ref.shape[0]):
            is_sink = is_sink | (lane == sink_ref[i])
        marks = jnp.where(sub == 0, 1.0, jnp.where((sub == 1) & is_sink, 1.0, 0.0))
        vt[g, hd : hd + EXTRA, :] = marks.astype(jnp.bfloat16)
        vtg = vt[g]
        pieces = []
        for h0 in range(0, width, 2):
            w = min(2, width - h0) * rows
            c0 = (g * width + h0) * rows
            pieces.append((w, slice(c0, c0 + w)))

        def scores(piece):
            w, cols = piece
            s = lax.dot_general(
                kp, qb[cols, :], (((1,), (1,)), ((), ())),
                preferred_element_type=jnp.float32,
            )
            if first:
                key_pos = base + lax.broadcasted_iota(jnp.int32, (span, w), 0)
                row = lax.broadcasted_iota(jnp.int32, (span, w), 1) % rows
                s = jnp.where(key_pos <= me * rows + row, s, NEG)
            return s

        ahead = scores(pieces[0])
        for j, (w, cols) in enumerate(pieces):
            s = ahead
            if j + 1 < len(pieces):
                ahead = scores(pieces[j + 1])
            top = jnp.max(s, axis=0, keepdims=True) * scale
            if first:
                new = top
            else:
                old = mref[:, cols]
                new = jnp.maximum(old, top)
            prob = jnp.exp2(s * scale - new).astype(jnp.bfloat16)
            part = jnp.dot(vtg, prob, preferred_element_type=jnp.float32)
            if first:
                acc[:, cols] = part
            else:
                acc[:, cols] = acc[:, cols] * jnp.exp2(old - new) + part
            mref[:, cols] = new

    @pl.when(z > 0)
    def _():
        take_z(z - 1)

    take_y(z)
    for h in range(heads):
        q_copy(h).wait()
    take_c(z)

    def step(p, first):
        for g in range(groups):
            compute(p, g, first)
            if g == 0:
                @pl.when(p > 1)
                def _():
                    take_z(p - 2)

                @pl.when(p > 0)
                def _():
                    take_y(p - 1)

        @pl.when(p > 0)
        def _():
            take_c(p - 1)

    step(z, True)

    def later(t, carry):
        step(z - t, False)
        return carry

    lax.fori_loop(1, z + 1, later, 0)

    length = len_ref[0]
    live = (me * rows + lax.broadcasted_iota(jnp.int32, (1, rows), 1)) < length
    stat_x[...] = jnp.zeros_like(stat_x)
    for h in range(heads):
        cols = slice(h * rows, (h + 1) * rows)
        total = acc[hd : hd + 1, cols]
        lse = (mref[:, cols] + jnp.log2(total)) * math.log(2.0)
        lse = jnp.where(live, lse, 0.0)
        mass = jnp.where(live, acc[hd + 1 : hd + 2, cols] / total, 0.0)
        rl_ref[h : h + 1, :] = lse
        sm_ref[h : h + 1, :] = mass
        stat_x[h : h + 1, :] = lse
        stat_x[64 + h : 65 + h, :] = mass
    sums = lax.dot_general(
        jnp.ones((8, rows), jnp.float32), stat_x[...], (((1,), (1,)), ((), ())),
        precision=lax.Precision.HIGHEST, preferred_element_type=jnp.float32,
    )
    stat_tx[...] = sums[0:1]

    def stat_copy(i):
        dev = (me + i) % n
        return pltpu.make_async_remote_copy(
            src_ref=stat_tx,
            dst_ref=stat_rx.at[me],
            send_sem=tsem.at[i],
            recv_sem=usem.at[me],
            device_id={"seq": dev},
            device_id_type=MESH,
        )

    def stat_from(i):
        src = (me + i) % n
        return pltpu.make_async_remote_copy(
            src_ref=stat_tx,
            dst_ref=stat_rx.at[src],
            send_sem=tsem.at[i],
            recv_sem=usem.at[src],
            device_id={"seq": src},
            device_id_type=MESH,
        )

    def stat_start(i, carry):
        stat_copy(i).start()
        return carry

    lax.fori_loop(1, n, stat_start, 0)

    for h in range(heads):
        cols = slice(h * rows, (h + 1) * rows)
        inv = jnp.where(live, 1.0 / acc[hd : hd + 1, cols], 0.0)
        out_ref[:, h * hd : (h + 1) * hd] = (acc[0:hd, cols] * inv).T.astype(jnp.bfloat16)

    def yc_done(p, carry):
        @pl.when(has_up)
        def _():
            for copy in move(block_id(p, y, c), up_dev, slot_z(p)):
                copy.wait_send()

        for copy in move(block_id(p, y, c), y_dev, slot_y(p)):
            copy.wait_send()
        for k in range(2):
            for copy in move(block_id(p, y, c), c_dev, slot_c(p, k)):
                copy.wait_send()
        return carry

    lax.fori_loop(0, z + 1, yc_done, 0)

    def stat_wait(i, carry):
        stat_copy(i).wait_send()
        stat_from(i).wait_recv()
        return carry

    lax.fori_loop(1, n, stat_wait, 0)
    stat_rx[pl.ds(me, 1)] = stat_tx[...].reshape(1, 1, rows)
    hd_ref[...] = jnp.sum(stat_rx[...], axis=0) / length.astype(jnp.float32)


def body(n, queries, keys, values, doc_length, sink_pos):
    rows, qcols = queries.shape
    kcols = keys.shape[1]
    heads = qcols // HEAD_DIMENSION
    groups = kcols // HEAD_DIMENSION
    planes = n // PLANE
    f32, bf16 = jnp.float32, jnp.bfloat16
    smem = pl.BlockSpec(memory_space=pltpu.SMEM)
    vmem = pl.BlockSpec(memory_space=pltpu.VMEM)
    hbm = pl.BlockSpec(memory_space=pl.ANY)
    attended, row_lse, sink_mass, head = pl.pallas_call(
        functools.partial(kernel, n, rows, heads, groups),
        out_shape=(
            jax.ShapeDtypeStruct((rows, qcols), bf16),
            jax.ShapeDtypeStruct((heads, rows), f32),
            jax.ShapeDtypeStruct((heads, rows), f32),
            jax.ShapeDtypeStruct((1, 128), f32),
        ),
        in_specs=[smem, smem, hbm, vmem, vmem],
        out_specs=(vmem, vmem, vmem, vmem),
        scratch_shapes=[
            pltpu.VMEM((heads * rows, HEAD_DIMENSION), bf16),
            pltpu.VMEM((n * rows, kcols), bf16),
            pltpu.VMEM((n * rows, kcols), bf16),
            pltpu.VMEM((groups, HEAD_DIMENSION + EXTRA, PLANE * rows), bf16),
            pltpu.VMEM((HEAD_DIMENSION + EXTRA, heads * rows), f32),
            pltpu.VMEM((1, heads * rows), f32),
            pltpu.VMEM((128, rows), f32),
            pltpu.VMEM((1, 128), f32),
            pltpu.VMEM((n, 1, 128), f32),
            pltpu.SemaphoreType.DMA((heads,)),
            pltpu.SemaphoreType.DMA((2, 4 * planes)),
            pltpu.SemaphoreType.DMA((2, n)),
            pltpu.SemaphoreType.DMA((n,)),
            pltpu.SemaphoreType.DMA((n,)),
        ],
        compiler_params=pltpu.CompilerParams(collective_id=0, has_side_effects=True, vmem_limit_bytes=(12 + n // 4) << 20
        ),
    )(doc_length, sink_pos, queries, keys, values)
    return attended, row_lse, sink_mass, head[0, :heads], head[0, 64 : 64 + heads]


def solution(mesh):
    placed = (
        P(("doc", "seq"), None),
        P(("doc", "seq"), None),
        P(("doc", "seq"), None),
        P("doc"),
        P("doc"),
    )
    return jax.shard_map(
        functools.partial(body, mesh.shape["seq"]),
        mesh=mesh,
        in_specs=placed,
        out_specs=(
            P(("doc", "seq"), None),
            P(None, ("doc", "seq")),
            P(None, ("doc", "seq")),
            P("doc"),
            P("doc"),
        ),
        check_vma=False,
    )
```

```python
import functools
import math

import jax
import jax.numpy as jnp
from jax import lax
from jax.experimental import pallas as pl
from jax.experimental.pallas import tpu as pltpu
from jax.sharding import PartitionSpec as P

HEAD_DIMENSION = 128
PLANE = 4
PARTS = 2
EXTRA = 16
MESH = pl.DeviceIdType.MESH
NEG = -1e30


def kernel(
    n, rows, heads, groups,
    len_ref, sink_ref, q_hbm, k_ref, v_ref,
    out_ref, st_ref,
    qb, kb, vb, vt, acc, mref, stat_x, stat_tx, stat_rx,
    qsem, ssem, rsem, lsem, tsem, usem,
):
    hd = HEAD_DIMENSION
    planes = n // PLANE
    span = 2 * rows
    width = heads // groups
    me = lax.axis_index("seq")
    z = me // PLANE
    y = (me // 2) % 2
    c = me % 2
    scale = (hd ** -0.5) * math.log2(math.e)

    def block_id(p, yy, cc):
        return p * PLANE + yy * 2 + cc

    def block(ref, b):
        return ref.at[pl.ds(pl.multiple_of(b * rows, rows), rows)]

    half = rows // PARTS

    def piece(buf, b, part):
        return buf.at[pl.ds(pl.multiple_of(b * rows + part * half, half), half)]

    def move(b, dev, slot):
        return [
            pltpu.make_async_remote_copy(
                src_ref=piece(buf, b, part),
                dst_ref=piece(buf, b, part),
                send_sem=ssem.at[kind * PARTS + part, slot],
                recv_sem=rsem.at[kind * PARTS + part, b],
                device_id={"seq": dev},
                device_id_type=MESH,
            )
            for kind, buf in enumerate((kb, vb))
            for part in range(PARTS)
        ]

    def arrive(b, dev):
        return move(b, dev, 0)

    def slot_z(p):
        return p

    def slot_y(p):
        return planes + p

    def slot_c(p, k):
        return 2 * planes + 2 * p + k

    y_dev = block_id(z, 1 - y, c)
    c_dev = block_id(z, y, 1 - c)

    loads = [
        pltpu.make_async_copy(src, block(buf, me), lsem.at[i])
        for i, (src, buf) in enumerate(((k_ref, kb), (v_ref, vb)))
    ]
    for load in loads:
        load.start()
    barrier = pltpu.get_barrier_semaphore()

    def greet(i, carry):
        pl.semaphore_signal(
            barrier, inc=1, device_id={"seq": (me + i) % n}, device_id_type=MESH
        )
        return carry

    lax.fori_loop(1, n, greet, 0)

    def q_copy(h):
        return pltpu.make_async_copy(
            q_hbm.at[:, pl.ds(h * hd, hd)], qb.at[pl.ds(h * rows, rows)], qsem.at[h]
        )

    for h in range(heads):
        q_copy(h).start()
    for load in loads:
        load.wait()
    pl.semaphore_wait(barrier, n - 1)

    up_dev = block_id(z + 1, y, c)
    has_up = z + 1 < planes

    @pl.when(has_up)
    def _():
        for copy in move(me, up_dev, slot_z(z)):
            copy.start()

    for copy in move(me, y_dev, slot_y(z)):
        copy.start()
    for copy in move(me, c_dev, slot_c(z, 0)):
        copy.start()

    def take_z(p):
        b = block_id(p, y, c)
        for got, to_z, to_y, to_c in zip(
            arrive(b, y_dev),
            move(b, up_dev, slot_z(p)),
            move(b, y_dev, slot_y(p)),
            move(b, c_dev, slot_c(p, 0)),
        ):
            got.wait_recv()
            pl.when(has_up)(to_z.start)
            to_y.start()
            to_c.start()

    def take_y(p):
        b = block_id(p, 1 - y, c)
        for got, to_c in zip(arrive(b, y_dev), move(b, c_dev, slot_c(p, 1))):
            got.wait_recv()
            to_c.start()

    def take_c(p, yy):
        for got in arrive(block_id(p, yy, 1 - c), c_dev):
            got.wait_recv()

    def compute(p, yy, g, first=False, masked=False):
        base = pl.multiple_of((p * 2 + yy) * span, span)
        kp = kb[pl.ds(base, span), g * hd : (g + 1) * hd]
        vt[g, 0:hd, :] = vb[pl.ds(base, span), g * hd : (g + 1) * hd].T
        lane = lax.broadcasted_iota(jnp.int32, (EXTRA, span), 1) + base
        sub = lax.broadcasted_iota(jnp.int32, (EXTRA, span), 0)
        is_sink = lane == sink_ref[0]
        for i in range(1, sink_ref.shape[0]):
            is_sink = is_sink | (lane == sink_ref[i])
        marks = jnp.where(sub == 0, 1.0, jnp.where((sub == 1) & is_sink, 1.0, 0.0))
        vt[g, hd : hd + EXTRA, :] = marks.astype(jnp.bfloat16)
        vtg = vt[g]
        pieces = []
        for h0 in range(0, width, 2):
            w = min(2, width - h0) * rows
            c0 = (g * width + h0) * rows
            pieces.append((w, slice(c0, c0 + w)))

        def scores(piece):
            w, cols = piece
            s = lax.dot_general(
                kp, qb[cols, :], (((1,), (1,)), ((), ())),
                preferred_element_type=jnp.float32,
            )
            if masked:
                key_pos = base + lax.broadcasted_iota(jnp.int32, (span, w), 0)
                row = lax.broadcasted_iota(jnp.int32, (span, w), 1) % rows
                s = jnp.where(key_pos <= me * rows + row, s, NEG)
            return s

        ahead = scores(pieces[0])
        for j, (w, cols) in enumerate(pieces):
            s = ahead
            if j + 1 < len(pieces):
                ahead = scores(pieces[j + 1])
            top = jnp.max(s, axis=0, keepdims=True) * scale
            if first:
                new = top
            else:
                old = mref[:, cols]
                new = jnp.maximum(old, top)
            prob = jnp.exp2(s * scale - new).astype(jnp.bfloat16)
            part = jnp.dot(vtg, prob, preferred_element_type=jnp.float32)
            if first:
                acc[:, cols] = part
            else:
                acc[:, cols] = acc[:, cols] * jnp.exp2(old - new) + part
            mref[:, cols] = new

    for h in range(heads):
        q_copy(h).wait()
    take_c(z, y)
    for g in range(groups):
        compute(z, y, g, first=True, masked=True)

    @pl.when(z > 0)
    def _():
        take_z(z - 1)

    take_y(z)

    def step(p, masked):
        @pl.when(p > 1)
        def _():
            take_z(p - 2)

        take_c(p, 1 - y)
        if masked:
            @pl.when(y == 1)
            def _():
                for g in range(groups):
                    compute(p, 1 - y, g, masked=True)
        else:
            for g in range(groups):
                compute(p, 1 - y, g)

        @pl.when(p > 0)
        def _():
            take_y(p - 1)
            take_c(p - 1, y)
            for g in range(groups):
                compute(p - 1, y, g)

    step(z, True)

    def later(t, carry):
        step(z - t, False)
        return carry

    lax.fori_loop(1, z + 1, later, 0)

    length = len_ref[0]
    live = (me * rows + lax.broadcasted_iota(jnp.int32, (1, rows), 1)) < length
    stat_x[...] = jnp.zeros_like(stat_x)
    for h in range(heads):
        cols = slice(h * rows, (h + 1) * rows)
        total = acc[hd : hd + 1, cols]
        lse = (mref[:, cols] + jnp.log2(total)) * math.log(2.0)
        lse = jnp.where(live, lse, 0.0)
        mass = jnp.where(live, acc[hd + 1 : hd + 2, cols] / total, 0.0)
        st_ref[h : h + 1, :] = lse
        st_ref[32 + h : 33 + h, :] = mass
        stat_x[h : h + 1, :] = lse
        stat_x[64 + h : 65 + h, :] = mass
    sums = lax.dot_general(
        jnp.ones((8, rows), jnp.float32), stat_x[...], (((1,), (1,)), ((), ())),
        precision=lax.Precision.HIGHEST, preferred_element_type=jnp.float32,
    )
    stat_tx[...] = sums[0:1]

    def stat_copy(i):
        dev = (me + i) % n
        return pltpu.make_async_remote_copy(
            src_ref=stat_tx,
            dst_ref=stat_rx.at[me],
            send_sem=tsem.at[i],
            recv_sem=usem.at[me],
            device_id={"seq": dev},
            device_id_type=MESH,
        )

    def stat_from(i):
        src = (me + i) % n
        return pltpu.make_async_remote_copy(
            src_ref=stat_tx,
            dst_ref=stat_rx.at[src],
            send_sem=tsem.at[i],
            recv_sem=usem.at[src],
            device_id={"seq": src},
            device_id_type=MESH,
        )

    def stat_start(i, carry):
        stat_copy(i).start()
        return carry

    lax.fori_loop(1, n, stat_start, 0)

    for h in range(heads):
        cols = slice(h * rows, (h + 1) * rows)
        inv = jnp.where(live, 1.0 / acc[hd : hd + 1, cols], 0.0)
        out_ref[:, h * hd : (h + 1) * hd] = (acc[0:hd, cols] * inv).T.astype(jnp.bfloat16)

    def yc_done(p, carry):
        @pl.when(has_up)
        def _():
            for copy in move(block_id(p, y, c), up_dev, slot_z(p)):
                copy.wait_send()

        for copy in move(block_id(p, y, c), y_dev, slot_y(p)):
            copy.wait_send()
        for k in range(2):
            for copy in move(block_id(p, y, c), c_dev, slot_c(p, k)):
                copy.wait_send()
        return carry

    lax.fori_loop(0, z + 1, yc_done, 0)

    def stat_wait(i, carry):
        stat_copy(i).wait_send()
        stat_from(i).wait_recv()
        return carry

    lax.fori_loop(1, n, stat_wait, 0)
    stat_rx[pl.ds(me, 1)] = stat_tx[...].reshape(1, 1, rows)
    st_ref[64:65, :] = jnp.sum(stat_rx[...], axis=0) / length.astype(jnp.float32)


def emit(heads, att_ref, st_ref, out_hbm, rl_ref, sm_ref, hl_ref, hs_ref, sem):
    copy = pltpu.make_async_copy(att_ref, out_hbm, sem)
    copy.start()
    rl_ref[...] = st_ref[0:heads]
    sm_ref[...] = st_ref[32 : 32 + heads]
    hl_ref[...] = st_ref[64, 0:heads]
    hs_ref[...] = st_ref[64, 64 : 64 + heads]
    copy.wait()


def body(n, queries, keys, values, doc_length, sink_pos):
    rows, qcols = queries.shape
    kcols = keys.shape[1]
    heads = qcols // HEAD_DIMENSION
    groups = kcols // HEAD_DIMENSION
    planes = n // PLANE
    f32, bf16 = jnp.float32, jnp.bfloat16
    smem = pl.BlockSpec(memory_space=pltpu.SMEM)
    vmem = pl.BlockSpec(memory_space=pltpu.VMEM)
    hbm = pl.BlockSpec(memory_space=pltpu.HBM)
    attended, stats = pl.pallas_call(
        functools.partial(kernel, n, rows, heads, groups),
        out_shape=(
            jax.ShapeDtypeStruct((rows, qcols), bf16),
            jax.ShapeDtypeStruct((72, rows), f32),
        ),
        in_specs=[smem, smem, hbm, hbm, hbm],
        out_specs=(vmem, vmem),
        scratch_shapes=[
            pltpu.VMEM((heads * rows, HEAD_DIMENSION), bf16),
            pltpu.VMEM((n * rows, kcols), bf16),
            pltpu.VMEM((n * rows, kcols), bf16),
            pltpu.VMEM((groups, HEAD_DIMENSION + EXTRA, 2 * rows), bf16),
            pltpu.VMEM((HEAD_DIMENSION + EXTRA, heads * rows), f32),
            pltpu.VMEM((1, heads * rows), f32),
            pltpu.VMEM((128, rows), f32),
            pltpu.VMEM((1, 128), f32),
            pltpu.VMEM((n, 1, 128), f32),
            pltpu.SemaphoreType.DMA((heads,)),
            pltpu.SemaphoreType.DMA((2 * PARTS, 4 * planes)),
            pltpu.SemaphoreType.DMA((2 * PARTS, n)),
            pltpu.SemaphoreType.DMA((2,)),
            pltpu.SemaphoreType.DMA((n,)),
            pltpu.SemaphoreType.DMA((n,)),
        ],
        compiler_params=pltpu.CompilerParams(collective_id=0, has_side_effects=True, vmem_limit_bytes=62 << 20
        ),
    )(doc_length, sink_pos, queries, keys, values)
    return pl.pallas_call(
        functools.partial(emit, heads),
        out_shape=(
            jax.ShapeDtypeStruct((rows, qcols), bf16),
            jax.ShapeDtypeStruct((heads, rows), f32),
            jax.ShapeDtypeStruct((heads, rows), f32),
            jax.ShapeDtypeStruct((heads,), f32),
            jax.ShapeDtypeStruct((heads,), f32),
        ),
        in_specs=[vmem, vmem],
        out_specs=(hbm, vmem, vmem, vmem, vmem),
        scratch_shapes=[pltpu.SemaphoreType.DMA],
        compiler_params=pltpu.CompilerParams(vmem_limit_bytes=4 << 20),
    )(attended, stats)


def solution(mesh):
    placed = (
        P(("doc", "seq"), None),
        P(("doc", "seq"), None),
        P(("doc", "seq"), None),
        P("doc"),
        P("doc"),
    )
    return jax.shard_map(
        functools.partial(body, mesh.shape["seq"]),
        mesh=mesh,
        in_specs=placed,
        out_specs=(
            P(("doc", "seq"), None),
            P(None, ("doc", "seq")),
            P(None, ("doc", "seq")),
            P("doc"),
            P("doc"),
        ),
        check_vma=False,
    )
```
